32 devices in a mesh: freq: 4 (over y, x), rows: 8 (over z, core).
Axes of the slice: x: 2, y: 2, z: 4, core: 2. Of those that a mesh axis runs over, the one named last changes fastest.
Arguments:
- coupling: bfloat16 [8192, 8192], P('rows'), may hold values from -1 to 1
- delays: int32 [8192, 8192], P('rows'), may hold values from 0 to 63
- freq_index: int32 [4], P('freq'), parts along dimension 0, may hold values from 0 to 255
- initial: float32 [4, 2, 8192], P('freq', None, 'rows'), parts along dimension 0, may hold values from -6 to 6
Outputs:
- eigvector: float32 [4, 2, 8192], P('freq', None, 'rows'), parts along dimension 0
- eigvalue: float32 [4, 2], P('freq'), parts along dimension 0
The draws below stay inside these ranges and needn't reach their ends.
There are 4 independent parts, one for each index of `freq`. The reference program is written for one: setup_inputs(seed, part) draws one part's arguments, and reference() takes and returns one part's arrays. A program takes and returns all parts, laid end to end along the dimension named above; an argument that names none is the same for every part. Nothing has to cross between parts.
All inputs are finite; a program needn't handle non-finite values.
Results may differ from the reference program's by a relative error of at most 0.0003.
Values sent between devices are 32-bit elements; how exact they have to be, the bound alone decides.
No kernel may reach another device: no remote copies, remote signals or barrier semaphores. Data moves between devices by JAX's collectives and lax.ppermute only.
A program may use at most 192 MiB of HBM per device.

```python
import math
import jax
import jax.numpy as jnp
from jax import lax

N = 8192
FTOTAL = 256
BINS = 64
ITERS = 4
FREQ = 1


def draw_coupling(key, part):
    first_key = jax.random.fold_in(key, 11)
    row_key = jax.random.fold_in(key, 12)
    column_key = jax.random.fold_in(key, 13)
    base = jnp.clip(jax.random.normal(first_key, (N, N), jnp.float32), -6.0, 6.0)
    position = jnp.arange(N, dtype=jnp.float32) / N
    row_factor = jnp.exp(0.5 * position * math.log(3.0) + jax.random.uniform(row_key, (N,), jnp.float32, 0.0, 0.5 * math.log(10.0)))
    column_factor = jnp.exp(jax.random.uniform(column_key, (N,), jnp.float32, 0.0, 0.5 * math.log(10.0)))
    spread = jnp.sqrt(jnp.mean(row_factor * row_factor) * jnp.mean(column_factor * column_factor) * N)
    weights = base * row_factor[:, None] * column_factor[None, :] / spread
    return weights.astype(jnp.bfloat16)


def place_ends(drawn, rng, least, high):
    spot = [jax.random.randint(jax.random.fold_in(rng, axis), (), 0, length) for axis, length in enumerate(drawn.shape)]
    longest = drawn.shape.index(max(drawn.shape))
    next_to = spot[:longest] + [(spot[longest] + 1) % drawn.shape[longest]] + spot[longest + 1:]
    return drawn.at[tuple(spot)].set(least).at[tuple(next_to)].set(high)


def block_scale(stream_key, extent, split, least, top_value):
    factor_of, own = 1.0, jax.random.fold_in(stream_key, 6)
    for dim, parts in split:
        heights = jnp.exp(jax.random.uniform(jax.random.fold_in(own, dim), (parts,), jnp.float32, least / len(split), top_value / len(split)))
        factor_of = factor_of * jnp.repeat(heights, extent[dim] // parts).reshape([-1 if axis == dim else 1 for axis in range(len(extent))])
    return factor_of


def normal_values(stream_key, shape, scale, limit, shards=(), kind=jnp.bfloat16):
    loudness = block_scale(stream_key, shape, shards, -0.22, 0.18) if shards else 1.0
    drawn = jax.random.normal(stream_key, shape, jnp.float32) * scale * loudness
    return jnp.minimum(jnp.maximum(drawn, -limit), limit).astype(kind)


def setup_inputs(seed: int = 0, part: int = 0) -> dict:
    streams_of = jax.random.split(jax.random.key(seed), 5)
    part_splits = jax.random.split(jax.random.fold_in(streams_of[4], part), 5)
    return {
        "coupling": draw_coupling(jax.random.fold_in(streams_of[4], 71), part),
        "delays": place_ends(jax.random.randint(streams_of[1], (N, N), 0, BINS), jax.random.fold_in(streams_of[1], 1), 0, BINS - 1).astype(jnp.int32),
        "freq_index": jax.random.randint(part_splits[2], (FREQ,), 0, FTOTAL).astype(jnp.int32),
        "initial": normal_values(part_splits[3], (FREQ, 2, N), 1.0, 6.0, ((2, 8),), jnp.float32),
    }


EPS = 1e-06

def product(real_part, imag_part, normed, own_rows, angular):
    real_prod = jnp.dot(real_part, normed.T, precision=lax.Precision.HIGHEST, preferred_element_type=jnp.float32)
    imag_prod = jnp.dot(imag_part, normed.T, precision=lax.Precision.HIGHEST, preferred_element_type=jnp.float32)
    new_real = real_prod[:, 0] - imag_prod[:, 1] - angular * own_rows[1]
    new_imag = real_prod[:, 1] + imag_prod[:, 0] + angular * own_rows[0]
    return jnp.stack([new_real, new_imag], axis=0)

def reference(coupling, delays, freq_index, initial):
    weights = coupling.astype(jnp.float32)

    def one_point(packed):
        which_freq, first = packed
        step_count = which_freq + 1
        residue = jnp.remainder(step_count * delays, 2 * FTOTAL)
        phase_angle = residue.astype(jnp.float32) * (math.pi / FTOTAL)
        real_part = -weights * jnp.cos(phase_angle)
        imag_part = weights * jnp.sin(phase_angle)
        angular = step_count.astype(jnp.float32) * (math.pi / FTOTAL)
        iterate = first
        previous = first
        for sweep in range(ITERS):
            squares = jnp.sum(iterate * iterate)
            normed = iterate / jnp.sqrt(squares / N + EPS)
            previous = normed
            iterate = product(real_part, imag_part, normed, normed, angular)
        squares = jnp.sum(iterate * iterate)
        result = iterate / jnp.sqrt(squares / N + EPS)
        dot_real = jnp.sum(previous[0] * iterate[0] + previous[1] * iterate[1]) / N
        dot_imag = jnp.sum(previous[0] * iterate[1] - previous[1] * iterate[0]) / N
        return (result, jnp.stack([dot_real, dot_imag]))
    eigvector, eigvalue = lax.map(one_point, (freq_index, initial))
    return (eigvector, eigvalue)
```

```python
import functools
import math

import jax
import jax.numpy as jnp
from jax import lax
from jax.experimental import pallas as pl
from jax.experimental.pallas import tpu as pltpu
from jax.sharding import PartitionSpec as P

FTOTAL = 256
ITERS = 4
EPS = 1e-06

F32 = jnp.float32
HIGH = jnp.bfloat16
LOW = jnp.float8_e4m3fn
SCALE = 2.0**17
VMEM = pl.BlockSpec(memory_space=pltpu.VMEM)
SMEM = pl.BlockSpec(memory_space=pltpu.SMEM)
ANY = pl.BlockSpec(memory_space=pl.ANY)
SUB, LANE, FINE = 8, 128, 8
GRANT = 8 * 2**20
CHUNK = 2048


def gather_rows(table, index):
    dims = lax.GatherDimensionNumbers(
        offset_dims=(),
        collapsed_slice_dims=(0,),
        start_index_map=(0,),
        operand_batching_dims=(1,),
        start_indices_batching_dims=(1,),
    )
    return lax.gather(
        table,
        index[..., None],
        dims,
        slice_sizes=(1, 1),
        mode=lax.GatherScatterMode.PROMISE_IN_BOUNDS,
    )


def tables(step_count):
    entry = lax.broadcasted_iota(jnp.int32, (SUB, LANE), 0)

    def angle(times):
        residue = (step_count * (entry * times)) & (2 * FTOTAL - 1)
        return residue.astype(F32) * (math.pi / FTOTAL)

    fine, coarse = angle(1), angle(FINE)
    fine_cos = jnp.cos(fine)
    fine_cos = jnp.where(jnp.abs(fine_cos) < 1e-6, 1e-6, fine_cos)
    return jnp.cos(coarse), jnp.sin(coarse), fine_cos * SCALE, jnp.sin(fine) / fine_cos


def build_operator(rows, strip, step_count, c_hbm, d_hbm, hi_ref, lo_ref, c_buf, d_buf, c_sem, d_sem):
    total, width = c_hbm.shape
    blocks = total // rows

    def copies(block, slot):
        here = pl.ds(pl.multiple_of(block * rows, rows), rows)
        return (
            pltpu.make_async_copy(c_hbm.at[here], c_buf.at[slot], c_sem.at[slot]),
            pltpu.make_async_copy(d_hbm.at[here], d_buf.at[slot], d_sem.at[slot]),
        )

    for copy in copies(0, 0):
        copy.start()
    coarse_cos, coarse_sin, fine_cos, fine_tan = tables(step_count)

    def block_body(block, carry):
        slot = lax.rem(block, 2)
        for copy in copies(block, slot):
            copy.wait()

        @pl.when(block + 1 < blocks)
        def _():
            for copy in copies(block + 1, 1 - slot):
                copy.start()

        def strip_body(at, carry):
            for row in range(0, rows, 32):
                for lane in range(0, strip, LANE):
                    here = pl.ds(pl.multiple_of(at * strip + lane, LANE), LANE)
                    weight = c_buf[slot, row : row + 32, here].astype(F32)
                    delay = d_buf[slot, row : row + 32, here]
                    reals, imags = [], []
                    for sub in range(0, 32, SUB):
                        bins = delay[sub : sub + SUB]
                        low, high = bins & (FINE - 1), bins >> 3
                        cos_l, tan_l = gather_rows(fine_cos, low), gather_rows(fine_tan, low)
                        cos_h, sin_h = gather_rows(coarse_cos, high), gather_rows(coarse_sin, high)
                        size = weight[sub : sub + SUB] * cos_l
                        reals.append(size * (cos_h - sin_h * tan_l))
                        imags.append(size * (sin_h + cos_h * tan_l))
                    to = pl.ds(pl.multiple_of(block * rows + row, 32), 32)
                    for plane, parts in ((0, reals), (1, imags)):
                        value = jnp.concatenate(parts, axis=0)
                        hi = value.astype(HIGH)
                        hi_ref[plane, to, here] = hi
                        lo_ref[plane, to, here] = (value - hi.astype(F32)).astype(LOW)
            return carry

        lax.fori_loop(0, width // strip, strip_body, 0)
        return carry

    lax.fori_loop(0, blocks, block_body, 0)


def split(value):
    first = value.astype(HIGH).astype(F32)
    second = (value - first).astype(HIGH).astype(F32)
    third = (value - first - second).astype(HIGH).astype(F32)
    return first, second, third


def advance(chunk, step_count, z_ref, hi_ref, lo_ref, left_c, left_s):
    peers, _, own = z_ref.shape
    nodes = peers * own
    whole = z_ref[0] * z_ref[0]
    for peer in range(1, peers):
        whole = whole + z_ref[peer] * z_ref[peer]
    squares = jnp.sum(jnp.sum(whole, axis=1, keepdims=True), axis=0, keepdims=True)
    inverse = 1.0 / jnp.sqrt(squares / nodes + EPS)
    for peer in range(peers):
        here = slice(peer * own, (peer + 1) * own)
        normed = z_ref[peer] * inverse
        turned = jnp.concatenate([-normed[1:2], normed[0:1]], axis=0)
        for left, value in ((left_c, -normed), (left_s, turned)):
            pad = jnp.zeros((16 - 6, own), F32)
            left[:, here] = jnp.concatenate([*split(value), pad], axis=0).astype(HIGH)

    def step(at, totals):
        here = pl.ds(pl.multiple_of(at * chunk, chunk), chunk)
        for plane, left in ((0, left_c), (1, left_s)):
            for matrix in (hi_ref, lo_ref):
                totals = totals + lax.dot_general(
                    left[:, here],
                    matrix[plane, :, here],
                    (((1,), (1,)), ((), ())),
                    preferred_element_type=F32,
                )
        return totals

    totals = lax.fori_loop(0, nodes // chunk, step, jnp.zeros((16, own), F32))
    product = (totals[0:2] + totals[2:4] + totals[4:6]) * (1.0 / SCALE)
    mine = z_ref[lax.axis_index("rows")] * inverse
    turned = jnp.concatenate([-mine[1:2], mine[0:1]], axis=0)
    angular = step_count.astype(F32) * (math.pi / FTOTAL)
    return mine, turned, product + angular * turned


def first_kernel(rows, strip, chunk, q_ref, z_hbm, c_hbm, d_hbm, out_ref, hi_ref, lo_ref, z_buf, left_c, left_s, z_sem, *scratch):
    fetch = pltpu.make_async_copy(z_hbm, z_buf, z_sem)
    fetch.start()
    step_count = q_ref[0] + 1
    build_operator(rows, strip, step_count, c_hbm, d_hbm, hi_ref, lo_ref, *scratch)
    fetch.wait()
    _, _, new = advance(chunk, step_count, z_buf, hi_ref, lo_ref, left_c, left_s)
    for peer in range(out_ref.shape[0]):
        out_ref[peer] = new


def next_kernel(chunk, q_ref, z_ref, hi_ref, lo_ref, out_ref, left_c, left_s):
    _, _, new = advance(chunk, q_ref[0] + 1, z_ref, hi_ref, lo_ref, left_c, left_s)
    for peer in range(out_ref.shape[0]):
        out_ref[peer] = new


def last_kernel(chunk, q_ref, z_ref, hi_ref, lo_ref, out_ref, sums_ref, left_c, left_s):
    mine, turned, new = advance(chunk, q_ref[0] + 1, z_ref, hi_ref, lo_ref, left_c, left_s)
    out_ref[...] = new

    def summed(value):
        return jnp.sum(jnp.sum(value, axis=1, keepdims=True), axis=0, keepdims=True)

    row = lax.broadcasted_iota(jnp.int32, (SUB, LANE), 0)
    sums = jnp.where(row == 0, summed(new * new), 0.0)
    sums = sums + jnp.where(row == 1, summed(mine * new), 0.0)
    sums = sums + jnp.where(row == 2, summed(turned * new), 0.0)
    for peer in range(sums_ref.shape[0]):
        sums_ref[peer] = sums


def first(step, z, coupling, delays):
    rows, strip = 64, 256
    total, width = coupling.shape
    shape = (2, total, width)
    return pl.pallas_call(
        functools.partial(first_kernel, rows, strip, min(CHUNK, width)),
        out_shape=(
            jax.ShapeDtypeStruct(z.shape, F32),
            pltpu.VMEM(shape, HIGH),
            pltpu.VMEM(shape, LOW),
        ),
        in_specs=[SMEM, ANY, ANY, ANY],
        out_specs=(VMEM, VMEM, VMEM),
        scratch_shapes=[
            pltpu.VMEM(z.shape, F32),
            pltpu.VMEM((16, width), HIGH),
            pltpu.VMEM((16, width), HIGH),
            pltpu.SemaphoreType.DMA,
            pltpu.VMEM((2, rows, width), coupling.dtype),
            pltpu.VMEM((2, rows, width), delays.dtype),
            pltpu.SemaphoreType.DMA((2,)),
            pltpu.SemaphoreType.DMA((2,)),
        ],
        compiler_params=pltpu.CompilerParams(vmem_limit_bytes=GRANT),
        name="first",
    )(step, z, coupling, delays)


def apply(kernel, outputs, step, z, hi, lo):
    nodes = z.shape[0] * z.shape[2]
    return pl.pallas_call(
        functools.partial(kernel, min(CHUNK, nodes)),
        out_shape=tuple(jax.ShapeDtypeStruct(shape, F32) for shape in outputs),
        in_specs=[SMEM, VMEM, VMEM, VMEM],
        out_specs=(VMEM,) * len(outputs),
        scratch_shapes=[pltpu.VMEM((16, nodes), HIGH), pltpu.VMEM((16, nodes), HIGH)],
        compiler_params=pltpu.CompilerParams(vmem_limit_bytes=GRANT),
        name="apply",
    )(step, z, hi, lo)


def finish_kernel(nodes, y_ref, sums_ref, vector_ref, value_ref):
    sums = jnp.sum(sums_ref[...], axis=0)
    vector_ref[...] = y_ref[...] * (1.0 / jnp.sqrt(sums[0:1, 0:1] / nodes + EPS))
    lane = lax.broadcasted_iota(jnp.int32, (1, LANE), 1)
    value_ref[...] = jnp.where(lane == 0, sums[1:2], sums[2:3]) * (1.0 / nodes)


def finish(nodes, y, sums):
    return pl.pallas_call(
        functools.partial(finish_kernel, nodes),
        out_shape=(jax.ShapeDtypeStruct(y.shape, F32), jax.ShapeDtypeStruct((1, LANE), F32)),
        in_specs=[VMEM, VMEM],
        out_specs=(VMEM, VMEM),
        name="finish",
    )(y, sums)


def exchange(value):
    return lax.all_to_all(value, "rows", 0, 0, tiled=True)


def solution(mesh):
    peers = mesh.shape["rows"]

    def point(coupling, delays, step, start):
        nodes = coupling.shape[1]
        z = exchange(jnp.broadcast_to(start[None], (peers, *start.shape)))
        y, hi, lo = first(step, z, coupling, delays)
        hi = pltpu.with_memory_space_constraint(hi, pltpu.VMEM)
        lo = pltpu.with_memory_space_constraint(lo, pltpu.VMEM)
        for sweep in range(1, ITERS - 1):
            (y,) = apply(next_kernel, [z.shape], step, exchange(y), hi, lo)
        y, sums = apply(last_kernel, [z.shape[1:], (peers, SUB, LANE)], step, exchange(y), hi, lo)
        return finish(nodes, y, exchange(sums))

    def shards(coupling, delays, freq_index, initial):
        vectors, values = [], []
        for at in range(freq_index.shape[0]):
            vector, value = point(coupling, delays, freq_index[at : at + 1], initial[at])
            vectors.append(vector)
            values.append(value[0, 0:2])
        return jnp.stack(vectors), jnp.stack(values)

    return jax.shard_map(
        shards,
        mesh=mesh,
        in_specs=(P("rows", None), P("rows", None), P("freq"), P("freq", None, "rows")),
        out_specs=(P("freq", None, "rows"), P("freq", None)),
        check_vma=False,
    )
```

```python
import functools
import math

import jax
import jax.numpy as jnp
from jax import lax
from jax.experimental import pallas as pl
from jax.experimental.pallas import tpu as pltpu
from jax.sharding import PartitionSpec as P

FTOTAL = 256
ITERS = 4
EPS = 1e-06

F32 = jnp.float32
HIGH = jnp.bfloat16
LOW = jnp.float8_e4m3fn
SCALE = 2.0**17
VMEM = pl.BlockSpec(memory_space=pltpu.VMEM)
SMEM = pl.BlockSpec(memory_space=pltpu.SMEM)
ANY = pl.BlockSpec(memory_space=pl.ANY)
SUB, LANE, FINE = 8, 128, 8
GRANT = 8 * 2**20
CHUNK = 2048
SLAB = 512


def gather_rows(table, index):
    dims = lax.GatherDimensionNumbers(
        offset_dims=(),
        collapsed_slice_dims=(0,),
        start_index_map=(0,),
        operand_batching_dims=(1,),
        start_indices_batching_dims=(1,),
    )
    return lax.gather(
        table,
        index[..., None],
        dims,
        slice_sizes=(1, 1),
        mode=lax.GatherScatterMode.PROMISE_IN_BOUNDS,
    )


def tables(step_count):
    entry = lax.broadcasted_iota(jnp.int32, (SUB, LANE), 0)

    def angle(times):
        residue = (step_count * (entry * times)) & (2 * FTOTAL - 1)
        return residue.astype(F32) * (math.pi / FTOTAL)

    fine, coarse = angle(1), angle(FINE)
    fine_cos = jnp.cos(fine)
    fine_cos = jnp.where(jnp.abs(fine_cos) < 1e-6, 1e-6, fine_cos)
    return jnp.cos(coarse), jnp.sin(coarse), fine_cos * SCALE, jnp.sin(fine) / fine_cos


def fill(step_tables, slab, c_buf, d_buf, hi_ref, lo_ref, at, rows):
    coarse_cos, coarse_sin, fine_cos, fine_tan = step_tables
    for lane in range(0, slab, LANE):
        highs, lows = ([], []), ([], [])
        for row in range(rows.start, rows.stop, 32):
            weight = c_buf[row : row + 32, lane : lane + LANE].astype(F32)
            delay = d_buf[row : row + 32, lane : lane + LANE]
            values = ([], [])
            for sub in range(0, 32, SUB):
                bins = delay[sub : sub + SUB]
                low, high = bins & (FINE - 1), bins >> 3
                cos_l, tan_l = gather_rows(fine_cos, low), gather_rows(fine_tan, low)
                cos_h, sin_h = gather_rows(coarse_cos, high), gather_rows(coarse_sin, high)
                size = weight[sub : sub + SUB] * cos_l
                values[0].append(size * (cos_h - sin_h * tan_l))
                values[1].append(size * (sin_h + cos_h * tan_l))
            for plane in range(2):
                value = jnp.concatenate(values[plane], axis=0)
                hi = value.astype(HIGH)
                highs[plane].append(hi)
                lows[plane].append((value - hi.astype(F32)).astype(LOW))
        to = pl.ds(pl.multiple_of(at + lane, LANE), LANE)
        for plane in range(2):
            hi_ref[plane, to, rows] = jnp.concatenate(highs[plane], axis=0).T
            lo_ref[plane, to, rows] = jnp.concatenate(lows[plane], axis=0).T


def multiply(left_c, left_s, hi_ref, lo_ref, here, rows):
    total = None
    for plane, left in ((0, left_c), (1, left_s)):
        for matrix in (hi_ref, lo_ref):
            part = jnp.dot(left[:, here], matrix[plane, here, rows], preferred_element_type=F32)
            total = part if total is None else total + part
    return total


def split(value):
    first = value.astype(HIGH).astype(F32)
    second = (value - first).astype(HIGH).astype(F32)
    third = (value - first - second).astype(HIGH).astype(F32)
    return first, second, third


def prepare(z_ref, left_c, left_s):
    peers, _, own = z_ref.shape
    whole = z_ref[0] * z_ref[0]
    for peer in range(1, peers):
        whole = whole + z_ref[peer] * z_ref[peer]
    squares = jnp.sum(jnp.sum(whole, axis=1, keepdims=True), axis=0, keepdims=True)
    inverse = 1.0 / jnp.sqrt(squares / (peers * own) + EPS)
    for peer in range(peers):
        here = slice(peer * own, (peer + 1) * own)
        normed = z_ref[peer] * inverse
        turned = jnp.concatenate([-normed[1:2], normed[0:1]], axis=0)
        for left, value in ((left_c, -normed), (left_s, turned)):
            pad = jnp.zeros((16 - 6, own), F32)
            left[:, here] = jnp.concatenate([*split(value), pad], axis=0).astype(HIGH)
    mine = z_ref[lax.axis_index("rows")] * inverse
    return mine, jnp.concatenate([-mine[1:2], mine[0:1]], axis=0)


def complete(step_count, totals, turned):
    product = (totals[0:2] + totals[2:4] + totals[4:6]) * (1.0 / SCALE)
    return product + step_count.astype(F32) * (math.pi / FTOTAL) * turned


def advance(chunk, step_count, z_ref, hi_ref, lo_ref, left_c, left_s):
    mine, turned = prepare(z_ref, left_c, left_s)
    nodes, own = hi_ref.shape[1:]

    def step(at, totals):
        here = pl.ds(pl.multiple_of(at * chunk, chunk), chunk)
        return totals + multiply(left_c, left_s, hi_ref, lo_ref, here, slice(0, own))

    totals = lax.fori_loop(0, nodes // chunk, step, jnp.zeros((16, own), F32))
    return mine, turned, complete(step_count, totals, turned)


def first_kernel(slab, q_ref, z_hbm, c_hbm, d_hbm, hi_ref, lo_ref, out_ref, z_buf, left_c, left_s, total, c_buf, d_buf, z_sem, c_sem, d_sem):
    own, nodes = c_hbm.shape
    slots = c_buf.shape[0]
    slabs = nodes // slab

    def copies(at, slot):
        here = pl.ds(pl.multiple_of(at * slab, slab), slab)
        return (
            pltpu.make_async_copy(c_hbm.at[:, here], c_buf.at[slot], c_sem.at[slot]),
            pltpu.make_async_copy(d_hbm.at[:, here], d_buf.at[slot], d_sem.at[slot]),
        )

    fetch = pltpu.make_async_copy(z_hbm, z_buf, z_sem)
    fetch.start()
    for at in range(min(slots - 1, slabs)):
        for copy in copies(at, at):
            copy.start()
    step_count = q_ref[0] + 1
    step_tables = tables(step_count)
    fetch.wait()
    _, turned = prepare(z_buf, left_c, left_s)
    total[...] = jnp.zeros_like(total)
    block = min(256, own)

    def body(at, carry):
        slot = lax.rem(at, slots)
        for copy in copies(at, slot):
            copy.wait()

        @pl.when(at + slots - 1 < slabs)
        def _():
            for copy in copies(at + slots - 1, lax.rem(at + slots - 1, slots)):
                copy.start()

        here = pl.ds(pl.multiple_of(at * slab, slab), slab)
        for row in range(0, own, block):
            rows = slice(row, row + block)
            fill(step_tables, slab, c_buf.at[slot], d_buf.at[slot], hi_ref, lo_ref, at * slab, rows)
            total[:, rows] += multiply(left_c, left_s, hi_ref, lo_ref, here, rows)
        return carry

    lax.fori_loop(0, slabs, body, 0)
    new = complete(step_count, total[...], turned)
    for peer in range(out_ref.shape[0]):
        out_ref[peer] = new


def next_kernel(chunk, q_ref, z_ref, hi_ref, lo_ref, out_ref, left_c, left_s):
    _, _, new = advance(chunk, q_ref[0] + 1, z_ref, hi_ref, lo_ref, left_c, left_s)
    for peer in range(out_ref.shape[0]):
        out_ref[peer] = new


def last_kernel(chunk, q_ref, z_ref, hi_ref, lo_ref, out_ref, sums_ref, left_c, left_s):
    mine, turned, new = advance(chunk, q_ref[0] + 1, z_ref, hi_ref, lo_ref, left_c, left_s)
    out_ref[...] = new

    def summed(value):
        return jnp.sum(jnp.sum(value, axis=1, keepdims=True), axis=0, keepdims=True)

    row = lax.broadcasted_iota(jnp.int32, (SUB, LANE), 0)
    sums = jnp.where(row == 0, summed(new * new), 0.0)
    sums = sums + jnp.where(row == 1, summed(mine * new), 0.0)
    sums = sums + jnp.where(row == 2, summed(turned * new), 0.0)
    for peer in range(sums_ref.shape[0]):
        sums_ref[peer] = sums


def first(step, z, coupling, delays):
    own, nodes = coupling.shape
    slab, slots = min(SLAB, nodes), 2
    shape = (2, nodes, own)
    return pl.pallas_call(
        functools.partial(first_kernel, slab),
        out_shape=(
            pltpu.VMEM(shape, HIGH),
            pltpu.VMEM(shape, LOW),
            pltpu.VMEM(z.shape, F32),
        ),
        in_specs=[SMEM, ANY, ANY, ANY],
        out_specs=(VMEM, VMEM, VMEM),
        scratch_shapes=[
            pltpu.VMEM(z.shape, F32),
            pltpu.VMEM((16, nodes), HIGH),
            pltpu.VMEM((16, nodes), HIGH),
            pltpu.VMEM((16, own), F32),
            pltpu.VMEM((slots, own, slab), coupling.dtype),
            pltpu.VMEM((slots, own, slab), delays.dtype),
            pltpu.SemaphoreType.DMA,
            pltpu.SemaphoreType.DMA((slots,)),
            pltpu.SemaphoreType.DMA((slots,)),
        ],
        compiler_params=pltpu.CompilerParams(vmem_limit_bytes=GRANT),
        name="first",
    )(step, z, coupling, delays)


def apply(kernel, outputs, step, z, hi, lo):
    nodes = z.shape[0] * z.shape[2]
    return pl.pallas_call(
        functools.partial(kernel, min(CHUNK, nodes)),
        out_shape=tuple(pltpu.VMEM(shape, F32) for shape in outputs),
        in_specs=[SMEM, VMEM, VMEM, VMEM],
        out_specs=(VMEM,) * len(outputs),
        scratch_shapes=[pltpu.VMEM((16, nodes), HIGH), pltpu.VMEM((16, nodes), HIGH)],
        compiler_params=pltpu.CompilerParams(vmem_limit_bytes=GRANT),
        name="apply",
    )(step, z, hi, lo)


def finish_kernel(nodes, y_ref, sums_ref, vector_ref, value_ref):
    sums = jnp.sum(sums_ref[...], axis=0)
    vector_ref[...] = y_ref[...] * (1.0 / jnp.sqrt(sums[0:1, 0:1] / nodes + EPS))
    lane = lax.broadcasted_iota(jnp.int32, (1, LANE), 1)
    value_ref[...] = jnp.where(lane == 0, sums[1:2], sums[2:3]) * (1.0 / nodes)


def finish(nodes, y, sums):
    return pl.pallas_call(
        functools.partial(finish_kernel, nodes),
        out_shape=(jax.ShapeDtypeStruct(y.shape, F32), jax.ShapeDtypeStruct((1, LANE), F32)),
        in_specs=[VMEM, VMEM],
        out_specs=(VMEM, VMEM),
        name="finish",
    )(y, sums)


def copies_of_all(value):
    return lax.all_to_all(value, "rows", 0, 0, tiled=True)


def exchange(value):
    return in_vmem(copies_of_all(value))


def in_vmem(value):
    return pltpu.with_memory_space_constraint(value, pltpu.VMEM)


def solution(mesh):
    peers = mesh.shape["rows"]

    def point(coupling, delays, step, start):
        nodes = coupling.shape[1]
        z = copies_of_all(jnp.broadcast_to(start[None], (peers, *start.shape)))
        hi, lo, y = first(step, z, coupling, delays)
        hi, lo = in_vmem(hi), in_vmem(lo)
        for sweep in range(1, ITERS - 1):
            (y,) = apply(next_kernel, [z.shape], step, exchange(y), hi, lo)
        y, sums = apply(last_kernel, [z.shape[1:], (peers, SUB, LANE)], step, exchange(y), hi, lo)
        return finish(nodes, y, exchange(sums))

    def shards(coupling, delays, freq_index, initial):
        vectors, values = [], []
        for at in range(freq_index.shape[0]):
            vector, value = point(coupling, delays, freq_index[at : at + 1], initial[at])
            vectors.append(vector)
            values.append(value[0, 0:2])
        return jnp.stack(vectors), jnp.stack(values)

    return jax.shard_map(
        shards,
        mesh=mesh,
        in_specs=(P("rows", None), P("rows", None), P("freq"), P("freq", None, "rows")),
        out_specs=(P("freq", None, "rows"), P("freq", None)),
        check_vma=False,
    )
```

```python
import functools
import math

import jax
import jax.numpy as jnp
from jax import lax
from jax.experimental import pallas as pl
from jax.experimental.pallas import tpu as pltpu
from jax.sharding import PartitionSpec as P

FTOTAL = 256
ITERS = 4
EPS = 1e-06

F32 = jnp.float32
HIGH = jnp.bfloat16
LOW = jnp.float8_e4m3fn
SCALE = 2.0**17
VMEM = pl.BlockSpec(memory_space=pltpu.VMEM)
SMEM = pl.BlockSpec(memory_space=pltpu.SMEM)
ANY = pl.BlockSpec(memory_space=pl.ANY)
SUB, LANE, FINE = 8, 128, 8
GRANT = 8 * 2**20
CHUNK = 2048
SLAB = 512


def gather_rows(table, index):
    dims = lax.GatherDimensionNumbers(
        offset_dims=(),
        collapsed_slice_dims=(0,),
        start_index_map=(0,),
        operand_batching_dims=(1,),
        start_indices_batching_dims=(1,),
    )
    return lax.gather(
        table,
        index[..., None],
        dims,
        slice_sizes=(1, 1),
        mode=lax.GatherScatterMode.PROMISE_IN_BOUNDS,
    )


def tables(step_count):
    entry = lax.broadcasted_iota(jnp.int32, (SUB, LANE), 0)

    def angle(times):
        residue = (step_count * (entry * times)) & (2 * FTOTAL - 1)
        return residue.astype(F32) * (math.pi / FTOTAL)

    fine, coarse = angle(1), angle(FINE)
    fine_cos = jnp.cos(fine)
    fine_cos = jnp.where(jnp.abs(fine_cos) < 1e-6, 1e-6, fine_cos)
    return jnp.cos(coarse), jnp.sin(coarse), fine_cos * SCALE, jnp.sin(fine) / fine_cos


def fill(table_ref, slab, c_buf, d_buf, hi_ref, lo_ref, at, rows):
    for lane in range(0, slab, LANE):
        for row in range(rows.start, rows.stop, LANE):
            fill_block(table_ref, c_buf, d_buf, hi_ref, lo_ref, at, lane, row)


def fill_block(table_ref, c_buf, d_buf, hi_ref, lo_ref, at, lane, row):
    coarse_cos, coarse_sin, fine_cos, fine_tan = (table_ref[i] for i in range(4))
    rows, lanes = slice(row, row + LANE), slice(lane, lane + LANE)
    weights = c_buf[rows, lanes].T.astype(F32)
    delays = d_buf[rows, lanes].T
    for first in range(0, LANE, 32):
        values = ([], [])
        for sub in range(first, first + 32, SUB):
            bins = delays[sub : sub + SUB]
            low, high = bins & (FINE - 1), bins >> 3
            cos_l, tan_l = gather_rows(fine_cos, low), gather_rows(fine_tan, low)
            cos_h, sin_h = gather_rows(coarse_cos, high), gather_rows(coarse_sin, high)
            size = weights[sub : sub + SUB] * cos_l
            values[0].append(size * (cos_h - sin_h * tan_l))
            values[1].append(size * (sin_h + cos_h * tan_l))
        to = pl.ds(pl.multiple_of(at + lane + first, 32), 32)
        for plane in range(2):
            value = jnp.concatenate(values[plane], axis=0)
            hi = value.astype(HIGH)
            hi_ref[plane, row // LANE, to, :] = hi
            lo_ref[plane, to, rows] = (value - hi.astype(F32)).astype(LOW)


def multiply(left_c, left_s, hi_ref, lo_ref, here, rows):
    total = None
    for plane, left in ((0, left_c), (1, left_s)):
        blocks = range(rows.start // LANE, rows.stop // LANE)
        high = jnp.concatenate([hi_ref[plane, block, here] for block in blocks], axis=1)
        for matrix in (high, lo_ref[plane, here, rows]):
            part = jnp.dot(left[:, here], matrix, preferred_element_type=F32)
            total = part if total is None else total + part
    return total


def split(value):
    first = value.astype(HIGH).astype(F32)
    second = (value - first).astype(HIGH).astype(F32)
    third = (value - first - second).astype(HIGH).astype(F32)
    return first, second, third


def prepare(z_ref, left_c, left_s):
    peers, _, own = z_ref.shape
    whole = z_ref[0] * z_ref[0]
    for peer in range(1, peers):
        whole = whole + z_ref[peer] * z_ref[peer]
    squares = jnp.sum(jnp.sum(whole, axis=1, keepdims=True), axis=0, keepdims=True)
    inverse = 1.0 / jnp.sqrt(squares / (peers * own) + EPS)
    for peer in range(peers):
        here = slice(peer * own, (peer + 1) * own)
        normed = z_ref[peer] * inverse
        turned = jnp.concatenate([-normed[1:2], normed[0:1]], axis=0)
        for left, value in ((left_c, -normed), (left_s, turned)):
            pad = jnp.zeros((16 - 6, own), F32)
            left[:, here] = jnp.concatenate([*split(value), pad], axis=0).astype(HIGH)
    mine = z_ref[lax.axis_index("rows")] * inverse
    return mine, jnp.concatenate([-mine[1:2], mine[0:1]], axis=0)


def complete(step_count, totals, turned):
    product = (totals[0:2] + totals[2:4] + totals[4:6]) * (1.0 / SCALE)
    return product + step_count.astype(F32) * (math.pi / FTOTAL) * turned


def advance(chunk, step_count, z_ref, hi_ref, lo_ref, left_c, left_s):
    mine, turned = prepare(z_ref, left_c, left_s)
    nodes, own = lo_ref.shape[1:]

    def step(at, totals):
        here = pl.ds(pl.multiple_of(at * chunk, chunk), chunk)
        return totals + multiply(left_c, left_s, hi_ref, lo_ref, here, slice(0, own))

    totals = lax.fori_loop(0, nodes // chunk, step, jnp.zeros((16, own), F32))
    return mine, turned, complete(step_count, totals, turned)


def first_kernel(slab, q_ref, z_hbm, c_hbm, d_hbm, hi_ref, lo_ref, out_ref, z_buf, left_c, left_s, total, table_ref, c_buf, d_buf, z_sem, c_sem, d_sem):
    own, nodes = c_hbm.shape
    slots = c_buf.shape[0]
    slabs = nodes // slab

    def copies(at, slot):
        here = pl.ds(pl.multiple_of(at * slab, slab), slab)
        return (
            pltpu.make_async_copy(c_hbm.at[:, here], c_buf.at[slot], c_sem.at[slot]),
            pltpu.make_async_copy(d_hbm.at[:, here], d_buf.at[slot], d_sem.at[slot]),
        )

    fetch = pltpu.make_async_copy(z_hbm, z_buf, z_sem)
    fetch.start()
    for at in range(min(slots - 1, slabs)):
        for copy in copies(at, at):
            copy.start()
    step_count = q_ref[0] + 1
    for at, table in enumerate(tables(step_count)):
        table_ref[at] = table
    fetch.wait()
    _, turned = prepare(z_buf, left_c, left_s)
    total[...] = jnp.zeros_like(total)
    block = min(256, own)

    def body(at, carry):
        slot = lax.rem(at, slots)
        for copy in copies(at, slot):
            copy.wait()

        @pl.when(at + slots - 1 < slabs)
        def _():
            for copy in copies(at + slots - 1, lax.rem(at + slots - 1, slots)):
                copy.start()

        here = pl.ds(pl.multiple_of(at * slab, slab), slab)
        for row in range(0, own, block):
            rows = slice(row, row + block)
            fill(table_ref, slab, c_buf.at[slot], d_buf.at[slot], hi_ref, lo_ref, at * slab, rows)
            total[:, rows] += multiply(left_c, left_s, hi_ref, lo_ref, here, rows)
        return carry

    lax.fori_loop(0, slabs, body, 0)
    new = complete(step_count, total[...], turned)
    for peer in range(out_ref.shape[0]):
        out_ref[peer] = new


def next_kernel(chunk, q_ref, z_ref, hi_ref, lo_ref, out_ref, left_c, left_s):
    _, _, new = advance(chunk, q_ref[0] + 1, z_ref, hi_ref, lo_ref, left_c, left_s)
    for peer in range(out_ref.shape[0]):
        out_ref[peer] = new


def last_kernel(chunk, q_ref, z_ref, hi_ref, lo_ref, out_ref, sums_ref, left_c, left_s):
    mine, turned, new = advance(chunk, q_ref[0] + 1, z_ref, hi_ref, lo_ref, left_c, left_s)
    out_ref[...] = new

    def summed(value):
        return jnp.sum(jnp.sum(value, axis=1, keepdims=True), axis=0, keepdims=True)

    row = lax.broadcasted_iota(jnp.int32, (SUB, LANE), 0)
    sums = jnp.where(row == 0, summed(new * new), 0.0)
    sums = sums + jnp.where(row == 1, summed(mine * new), 0.0)
    sums = sums + jnp.where(row == 2, summed(turned * new), 0.0)
    for peer in range(sums_ref.shape[0]):
        sums_ref[peer] = sums


def first(step, z, coupling, delays):
    own, nodes = coupling.shape
    slab, slots = min(SLAB, nodes), 2
    return pl.pallas_call(
        functools.partial(first_kernel, slab),
        out_shape=(
            pltpu.VMEM((2, own // LANE, nodes, LANE), HIGH),
            pltpu.VMEM((2, nodes, own), LOW),
            pltpu.VMEM(z.shape, F32),
        ),
        in_specs=[SMEM, ANY, ANY, ANY],
        out_specs=(VMEM, VMEM, VMEM),
        scratch_shapes=[
            pltpu.VMEM(z.shape, F32),
            pltpu.VMEM((16, nodes), HIGH),
            pltpu.VMEM((16, nodes), HIGH),
            pltpu.VMEM((16, own), F32),
            pltpu.VMEM((4, SUB, LANE), F32),
            pltpu.VMEM((slots, own, slab), coupling.dtype),
            pltpu.VMEM((slots, own, slab), delays.dtype),
            pltpu.SemaphoreType.DMA,
            pltpu.SemaphoreType.DMA((slots,)),
            pltpu.SemaphoreType.DMA((slots,)),
        ],
        compiler_params=pltpu.CompilerParams(vmem_limit_bytes=GRANT),
        name="first",
    )(step, z, coupling, delays)


def apply(kernel, outputs, step, z, hi, lo):
    nodes = z.shape[0] * z.shape[2]
    return pl.pallas_call(
        functools.partial(kernel, min(CHUNK, nodes)),
        out_shape=tuple(pltpu.VMEM(shape, F32) for shape in outputs),
        in_specs=[SMEM, VMEM, VMEM, VMEM],
        out_specs=(VMEM,) * len(outputs),
        scratch_shapes=[pltpu.VMEM((16, nodes), HIGH), pltpu.VMEM((16, nodes), HIGH)],
        compiler_params=pltpu.CompilerParams(vmem_limit_bytes=GRANT),
        name="apply",
    )(step, z, hi, lo)


def finish_kernel(nodes, y_ref, sums_ref, vector_ref, value_ref):
    sums = jnp.sum(sums_ref[...], axis=0)
    vector_ref[...] = y_ref[...] * (1.0 / jnp.sqrt(sums[0:1, 0:1] / nodes + EPS))
    lane = lax.broadcasted_iota(jnp.int32, (1, LANE), 1)
    value_ref[...] = jnp.where(lane == 0, sums[1:2], sums[2:3]) * (1.0 / nodes)


def finish(nodes, y, sums):
    return pl.pallas_call(
        functools.partial(finish_kernel, nodes),
        out_shape=(jax.ShapeDtypeStruct(y.shape, F32), jax.ShapeDtypeStruct((1, LANE), F32)),
        in_specs=[VMEM, VMEM],
        out_specs=(VMEM, VMEM),
        name="finish",
    )(y, sums)


def copies_of_all(value):
    return lax.all_to_all(value, "rows", 0, 0, tiled=True)


def exchange(value):
    return in_vmem(copies_of_all(value))


def in_vmem(value):
    return pltpu.with_memory_space_constraint(value, pltpu.VMEM)


def solution(mesh):
    peers = mesh.shape["rows"]

    def point(coupling, delays, step, start):
        nodes = coupling.shape[1]
        z = copies_of_all(jnp.broadcast_to(start[None], (peers, *start.shape)))
        hi, lo, y = first(step, z, coupling, delays)
        hi, lo = in_vmem(hi), in_vmem(lo)
        for sweep in range(1, ITERS - 1):
            (y,) = apply(next_kernel, [z.shape], step, exchange(y), hi, lo)
        y, sums = apply(last_kernel, [z.shape[1:], (peers, SUB, LANE)], step, exchange(y), hi, lo)
        return finish(nodes, y, exchange(sums))

    def shards(coupling, delays, freq_index, initial):
        vectors, values = [], []
        for at in range(freq_index.shape[0]):
            vector, value = point(coupling, delays, freq_index[at : at + 1], initial[at])
            vectors.append(vector)
            values.append(value[0, 0:2])
        return jnp.stack(vectors), jnp.stack(values)

    return jax.shard_map(
        shards,
        mesh=mesh,
        in_specs=(P("rows", None), P("rows", None), P("freq"), P("freq", None, "rows")),
        out_specs=(P("freq", None, "rows"), P("freq", None)),
        check_vma=False,
    )
```

```python
import functools
import math

import jax
import jax.numpy as jnp
from jax import lax
from jax.experimental import pallas as pl
from jax.experimental.pallas import tpu as pltpu
from jax.sharding import PartitionSpec as P

FTOTAL = 256
ITERS = 4
EPS = 1e-06

F32 = jnp.float32
HIGH = jnp.bfloat16
LOW = jnp.float8_e4m3fn
SCALE = 2.0**17
VMEM = pl.BlockSpec(memory_space=pltpu.VMEM)
SMEM = pl.BlockSpec(memory_space=pltpu.SMEM)
ANY = pl.BlockSpec(memory_space=pl.ANY)
SUB, LANE, FINE = 8, 128, 8
GRANT = 17 * 2**19
CHUNK = 4096
SLAB = 512


def gather_rows(table, index):
    dims = lax.GatherDimensionNumbers(
        offset_dims=(),
        collapsed_slice_dims=(0,),
        start_index_map=(0,),
        operand_batching_dims=(1,),
        start_indices_batching_dims=(1,),
    )
    return lax.gather(
        table,
        index[..., None],
        dims,
        slice_sizes=(1, 1),
        mode=lax.GatherScatterMode.PROMISE_IN_BOUNDS,
    )


def tables(step_count):
    entry = lax.broadcasted_iota(jnp.int32, (SUB, LANE), 0)

    def angle(times):
        residue = (step_count * (entry * times)) & (2 * FTOTAL - 1)
        return residue.astype(F32) * (math.pi / FTOTAL)

    fine, coarse = angle(1), angle(FINE)
    fine_cos = jnp.cos(fine)
    fine_cos = jnp.where(jnp.abs(fine_cos) < 1e-6, 1e-6, fine_cos)
    return jnp.cos(coarse), jnp.sin(coarse), fine_cos * SCALE, jnp.sin(fine) / fine_cos


def fill(table_ref, slab, c_buf, d_buf, hi_ref, lo_ref, at, rows):
    for lane in range(0, slab, LANE):
        for row in range(rows.start, rows.stop, LANE):
            fill_block(table_ref, c_buf, d_buf, hi_ref, lo_ref, at, lane, row)


def fill_block(table_ref, c_buf, d_buf, hi_ref, lo_ref, at, lane, row):
    coarse_cos, coarse_sin, fine_cos, fine_tan = (table_ref[i] for i in range(4))
    rows, lanes = slice(row, row + LANE), slice(lane, lane + LANE)
    weights = c_buf[rows, lanes].T.astype(F32)
    delays = d_buf[rows, lanes].T
    for first in range(0, LANE, 32):
        values = ([], [])
        for sub in range(first, first + 32, SUB):
            bins = delays[sub : sub + SUB]
            low, high = bins & (FINE - 1), bins >> 3
            cos_l, tan_l = gather_rows(fine_cos, low), gather_rows(fine_tan, low)
            cos_h, sin_h = gather_rows(coarse_cos, high), gather_rows(coarse_sin, high)
            size = weights[sub : sub + SUB] * cos_l
            values[0].append(size * (cos_h - sin_h * tan_l))
            values[1].append(size * (sin_h + cos_h * tan_l))
        to = pl.ds(pl.multiple_of(at + lane + first, 32), 32)
        for plane in range(2):
            value = jnp.concatenate(values[plane], axis=0)
            hi = value.astype(HIGH)
            hi_ref[plane, row // LANE, to, :] = hi
            lo_ref[plane, to, rows] = (value - hi.astype(F32)).astype(LOW)


def multiply(left_c, left_s, hi_ref, lo_ref, here, rows):
    total = None
    for plane, left in ((0, left_c), (1, left_s)):
        blocks = range(rows.start // LANE, rows.stop // LANE)
        high = jnp.concatenate([hi_ref[plane, block, here] for block in blocks], axis=1)
        for matrix in (high, lo_ref[plane, here, rows]):
            part = jnp.dot(left[:, here], matrix, preferred_element_type=F32)
            total = part if total is None else total + part
    return total


def split(value):
    first = value.astype(HIGH).astype(F32)
    second = (value - first).astype(HIGH).astype(F32)
    third = (value - first - second).astype(HIGH).astype(F32)
    return first, second, third


def prepare(z_ref, left_c, left_s):
    peers, _, own = z_ref.shape
    whole = z_ref[0] * z_ref[0]
    for peer in range(1, peers):
        whole = whole + z_ref[peer] * z_ref[peer]
    squares = jnp.sum(jnp.sum(whole, axis=1, keepdims=True), axis=0, keepdims=True)
    inverse = 1.0 / jnp.sqrt(squares / (peers * own) + EPS)
    for peer in range(peers):
        here = slice(peer * own, (peer + 1) * own)
        normed = z_ref[peer] * inverse
        turned = jnp.concatenate([-normed[1:2], normed[0:1]], axis=0)
        for left, value in ((left_c, -normed), (left_s, turned)):
            pad = jnp.zeros((16 - 6, own), F32)
            left[:, here] = jnp.concatenate([*split(value), pad], axis=0).astype(HIGH)
    mine = z_ref[lax.axis_index("rows")] * inverse
    return mine, jnp.concatenate([-mine[1:2], mine[0:1]], axis=0)


def complete(step_count, totals, turned):
    product = (totals[0:2] + totals[2:4] + totals[4:6]) * (1.0 / SCALE)
    return product + step_count.astype(F32) * (math.pi / FTOTAL) * turned


def advance(chunk, step_count, z_ref, hi_ref, lo_ref, left_c, left_s):
    mine, turned = prepare(z_ref, left_c, left_s)
    nodes, own = lo_ref.shape[1:]

    def step(at, totals):
        here = pl.ds(pl.multiple_of(at * chunk, chunk), chunk)
        return totals + multiply(left_c, left_s, hi_ref, lo_ref, here, slice(0, own))

    totals = lax.fori_loop(0, nodes // chunk, step, jnp.zeros((16, own), F32))
    return mine, turned, complete(step_count, totals, turned)


def first_kernel(slab, q_ref, z_ref, c_hbm, d_hbm, hi_ref, lo_ref, out_ref, left_c, left_s, total, table_ref, c_buf, d_buf, c_sem, d_sem):
    own, nodes = c_hbm.shape
    slots = c_buf.shape[0]
    slabs = nodes // slab

    def copies(at, slot):
        here = pl.ds(pl.multiple_of(at * slab, slab), slab)
        return (
            pltpu.make_async_copy(c_hbm.at[:, here], c_buf.at[slot], c_sem.at[slot]),
            pltpu.make_async_copy(d_hbm.at[:, here], d_buf.at[slot], d_sem.at[slot]),
        )

    for at in range(min(slots - 1, slabs)):
        for copy in copies(at, at):
            copy.start()
    step_count = q_ref[0] + 1
    for at, table in enumerate(tables(step_count)):
        table_ref[at] = table
    _, turned = prepare(z_ref, left_c, left_s)
    total[...] = jnp.zeros_like(total)
    block = min(256, own)

    def body(at, carry):
        slot = lax.rem(at, slots)
        for copy in copies(at, slot):
            copy.wait()

        @pl.when(at + slots - 1 < slabs)
        def _():
            for copy in copies(at + slots - 1, lax.rem(at + slots - 1, slots)):
                copy.start()

        here = pl.ds(pl.multiple_of(at * slab, slab), slab)
        for row in range(0, own, block):
            rows = slice(row, row + block)
            fill(table_ref, slab, c_buf.at[slot], d_buf.at[slot], hi_ref, lo_ref, at * slab, rows)
            total[:, rows] += multiply(left_c, left_s, hi_ref, lo_ref, here, rows)
        return carry

    lax.fori_loop(0, slabs, body, 0)
    new = complete(step_count, total[...], turned)
    for peer in range(out_ref.shape[0]):
        out_ref[peer] = new


def next_kernel(chunk, q_ref, z_ref, hi_ref, lo_ref, out_ref, left_c, left_s):
    _, _, new = advance(chunk, q_ref[0] + 1, z_ref, hi_ref, lo_ref, left_c, left_s)
    for peer in range(out_ref.shape[0]):
        out_ref[peer] = new


def last_kernel(chunk, q_ref, z_ref, hi_ref, lo_ref, out_ref, sums_ref, left_c, left_s):
    mine, turned, new = advance(chunk, q_ref[0] + 1, z_ref, hi_ref, lo_ref, left_c, left_s)
    out_ref[...] = new

    def summed(value):
        return jnp.sum(jnp.sum(value, axis=1, keepdims=True), axis=0, keepdims=True)

    row = lax.broadcasted_iota(jnp.int32, (SUB, LANE), 0)
    sums = jnp.where(row == 0, summed(new * new), 0.0)
    sums = sums + jnp.where(row == 1, summed(mine * new), 0.0)
    sums = sums + jnp.where(row == 2, summed(turned * new), 0.0)
    for peer in range(sums_ref.shape[0]):
        sums_ref[peer] = sums


def first(step, z, coupling, delays):
    own, nodes = coupling.shape
    slab, slots = min(SLAB, nodes), 2
    return pl.pallas_call(
        functools.partial(first_kernel, slab),
        out_shape=(
            pltpu.VMEM((2, own // LANE, nodes, LANE), HIGH),
            pltpu.VMEM((2, nodes, own), LOW),
            pltpu.VMEM(z.shape, F32),
        ),
        in_specs=[SMEM, VMEM, ANY, ANY],
        out_specs=(VMEM, VMEM, VMEM),
        scratch_shapes=[
            pltpu.VMEM((16, nodes), HIGH),
            pltpu.VMEM((16, nodes), HIGH),
            pltpu.VMEM((16, own), F32),
            pltpu.VMEM((4, SUB, LANE), F32),
            pltpu.VMEM((slots, own, slab), coupling.dtype),
            pltpu.VMEM((slots, own, slab), delays.dtype),
            pltpu.SemaphoreType.DMA((slots,)),
            pltpu.SemaphoreType.DMA((slots,)),
        ],
        compiler_params=pltpu.CompilerParams(vmem_limit_bytes=GRANT - 4 * math.prod(z.shape)),
        name="first",
    )(step, z, coupling, delays)


def apply(kernel, outputs, step, z, hi, lo):
    nodes = z.shape[0] * z.shape[2]
    return pl.pallas_call(
        functools.partial(kernel, min(CHUNK, nodes)),
        out_shape=tuple(pltpu.VMEM(shape, F32) for shape in outputs),
        in_specs=[SMEM, VMEM, VMEM, VMEM],
        out_specs=(VMEM,) * len(outputs),
        scratch_shapes=[pltpu.VMEM((16, nodes), HIGH), pltpu.VMEM((16, nodes), HIGH)],
        compiler_params=pltpu.CompilerParams(vmem_limit_bytes=GRANT),
        name="apply",
    )(step, z, hi, lo)


def finish_kernel(nodes, y_ref, sums_ref, vector_ref, value_ref):
    sums = jnp.sum(sums_ref[...], axis=0)
    vector_ref[...] = y_ref[...] * (1.0 / jnp.sqrt(sums[0:1, 0:1] / nodes + EPS))
    lane = lax.broadcasted_iota(jnp.int32, (1, LANE), 1)
    value_ref[...] = jnp.where(lane == 0, sums[1:2], sums[2:3]) * (1.0 / nodes)


def finish(nodes, y, sums):
    return pl.pallas_call(
        functools.partial(finish_kernel, nodes),
        out_shape=(jax.ShapeDtypeStruct(y.shape, F32), jax.ShapeDtypeStruct((1, LANE), F32)),
        in_specs=[VMEM, VMEM],
        out_specs=(VMEM, VMEM),
        name="finish",
    )(y, sums)


def copies_of_all(value):
    return lax.all_to_all(value, "rows", 0, 0, tiled=True)


def exchange(value):
    return in_vmem(copies_of_all(value))


def in_vmem(value):
    return pltpu.with_memory_space_constraint(value, pltpu.VMEM)


def solution(mesh):
    peers = mesh.shape["rows"]

    def point(coupling, delays, step, start):
        nodes = coupling.shape[1]
        z = exchange(jnp.broadcast_to(start[None], (peers, *start.shape)))
        hi, lo, y = first(step, z, coupling, delays)
        hi, lo = in_vmem(hi), in_vmem(lo)
        for sweep in range(1, ITERS - 1):
            (y,) = apply(next_kernel, [z.shape], step, exchange(y), hi, lo)
        y, sums = apply(last_kernel, [z.shape[1:], (peers, SUB, LANE)], step, exchange(y), hi, lo)
        return finish(nodes, y, exchange(sums))

    def shards(coupling, delays, freq_index, initial):
        vectors, values = [], []
        for at in range(freq_index.shape[0]):
            vector, value = point(coupling, delays, freq_index[at : at + 1], initial[at])
            vectors.append(vector)
            values.append(value[0, 0:2])
        return jnp.stack(vectors), jnp.stack(values)

    return jax.shard_map(
        shards,
        mesh=mesh,
        in_specs=(P("rows", None), P("rows", None), P("freq"), P("freq", None, "rows")),
        out_specs=(P("freq", None, "rows"), P("freq", None)),
        check_vma=False,
    )
```

```python
import functools
import math

import jax
import jax.numpy as jnp
from jax import lax
from jax.experimental import pallas as pl
from jax.experimental.pallas import tpu as pltpu
from jax.sharding import PartitionSpec as P

FTOTAL = 256
ITERS = 4
EPS = 1e-06

F32 = jnp.float32
HIGH = jnp.bfloat16
LOW = jnp.float8_e4m3fn
SCALE = 2.0**17
VMEM = pl.BlockSpec(memory_space=pltpu.VMEM)
SMEM = pl.BlockSpec(memory_space=pltpu.SMEM)
ANY = pl.BlockSpec(memory_space=pl.ANY)
SUB, LANE, FINE = 8, 128, 8
GRANT = 17 * 2**19
CHUNK = 8192
SLAB = 512


def gather_rows(table, index):
    dims = lax.GatherDimensionNumbers(
        offset_dims=(),
        collapsed_slice_dims=(0,),
        start_index_map=(0,),
        operand_batching_dims=(1,),
        start_indices_batching_dims=(1,),
    )
    return lax.gather(
        table,
        index[..., None],
        dims,
        slice_sizes=(1, 1),
        mode=lax.GatherScatterMode.PROMISE_IN_BOUNDS,
    )


def tables(step_count):
    entry = lax.broadcasted_iota(jnp.int32, (SUB, LANE), 0)

    def angle(times):
        residue = (step_count * (entry * times)) & (2 * FTOTAL - 1)
        return residue.astype(F32) * (math.pi / FTOTAL)

    fine, coarse = angle(1), angle(FINE)
    fine_cos = jnp.cos(fine)
    fine_cos = jnp.where(jnp.abs(fine_cos) < 1e-6, 1e-6, fine_cos)
    return jnp.cos(coarse), jnp.sin(coarse), fine_cos * SCALE, jnp.sin(fine) / fine_cos


def fill(table_ref, slab, c_buf, d_buf, hi_ref, lo_ref, at, rows):
    for lane in range(0, slab, LANE):
        for row in range(rows.start, rows.stop, LANE):
            fill_block(table_ref, c_buf, d_buf, hi_ref, lo_ref, at, lane, row)


def fill_block(table_ref, c_buf, d_buf, hi_ref, lo_ref, at, lane, row):
    coarse_cos, coarse_sin, fine_cos, fine_tan = (table_ref[i] for i in range(4))
    rows, lanes = slice(row, row + LANE), slice(lane, lane + LANE)
    weights = c_buf[rows, lanes].T.astype(F32)
    delays = d_buf[rows, lanes].T
    for first in range(0, LANE, 32):
        values = ([], [])
        for sub in range(first, first + 32, SUB):
            bins = delays[sub : sub + SUB]
            low, high = bins & (FINE - 1), bins >> 3
            cos_l, tan_l = gather_rows(fine_cos, low), gather_rows(fine_tan, low)
            cos_h, sin_h = gather_rows(coarse_cos, high), gather_rows(coarse_sin, high)
            size = weights[sub : sub + SUB] * cos_l
            values[0].append(size * (cos_h - sin_h * tan_l))
            values[1].append(size * (sin_h + cos_h * tan_l))
        to = pl.ds(pl.multiple_of(at + lane + first, 32), 32)
        for plane in range(2):
            value = jnp.concatenate(values[plane], axis=0)
            hi = value.astype(HIGH)
            hi_ref[plane, row // LANE, to, :] = hi
            lo_ref[plane, to, rows] = (value - hi.astype(F32)).astype(LOW)


def multiply(left_c, left_s, hi_ref, lo_ref, here, rows):
    total = None
    for plane, left in ((0, left_c), (1, left_s)):
        blocks = range(rows.start // LANE, rows.stop // LANE)
        high = jnp.concatenate([hi_ref[plane, block, here] for block in blocks], axis=1)
        for matrix in (high, lo_ref[plane, here, rows]):
            part = jnp.dot(left[:, here], matrix, preferred_element_type=F32)
            total = part if total is None else total + part
    return total


def split(value):
    first = value.astype(HIGH).astype(F32)
    second = (value - first).astype(HIGH).astype(F32)
    third = (value - first - second).astype(HIGH).astype(F32)
    return first, second, third


def prepare(z_ref, left_c, left_s):
    peers, _, own = z_ref.shape
    whole = z_ref[0] * z_ref[0]
    for peer in range(1, peers):
        whole = whole + z_ref[peer] * z_ref[peer]
    squares = jnp.sum(jnp.sum(whole, axis=1, keepdims=True), axis=0, keepdims=True)
    inverse = 1.0 / jnp.sqrt(squares / (peers * own) + EPS)
    for peer in range(peers):
        here = slice(peer * own, (peer + 1) * own)
        normed = z_ref[peer] * inverse
        turned = jnp.concatenate([-normed[1:2], normed[0:1]], axis=0)
        for left, value in ((left_c, -normed), (left_s, turned)):
            pad = jnp.zeros((16 - 6, own), F32)
            left[:, here] = jnp.concatenate([*split(value), pad], axis=0).astype(HIGH)
    mine = z_ref[lax.axis_index("rows")] * inverse
    return mine, jnp.concatenate([-mine[1:2], mine[0:1]], axis=0)


def complete(step_count, totals, turned):
    product = (totals[0:2] + totals[2:4] + totals[4:6]) * (1.0 / SCALE)
    return product + step_count.astype(F32) * (math.pi / FTOTAL) * turned


def advance(chunk, step_count, z_ref, hi_ref, lo_ref, left_c, left_s):
    mine, turned = prepare(z_ref, left_c, left_s)
    nodes, own = lo_ref.shape[1:]

    def step(at, totals):
        here = pl.ds(pl.multiple_of(at * chunk, chunk), chunk)
        return totals + multiply(left_c, left_s, hi_ref, lo_ref, here, slice(0, own))

    totals = lax.fori_loop(0, nodes // chunk, step, jnp.zeros((16, own), F32))
    return mine, turned, complete(step_count, totals, turned)


def first_kernel(slab, q_ref, z_ref, c_hbm, d_hbm, hi_ref, lo_ref, out_ref, left_c, left_s, total, table_ref, c_buf, d_buf, c_sem, d_sem):
    own, nodes = c_hbm.shape
    slots = c_buf.shape[0]
    slabs = nodes // slab

    def copies(at, slot):
        here = pl.ds(pl.multiple_of(at * slab, slab), slab)
        return (
            pltpu.make_async_copy(c_hbm.at[:, here], c_buf.at[slot], c_sem.at[slot]),
            pltpu.make_async_copy(d_hbm.at[:, here], d_buf.at[slot], d_sem.at[slot]),
        )

    for at in range(min(slots - 1, slabs)):
        for copy in copies(at, at):
            copy.start()
    step_count = q_ref[0] + 1
    for at, table in enumerate(tables(step_count)):
        table_ref[at] = table
    _, turned = prepare(z_ref, left_c, left_s)
    total[...] = jnp.zeros_like(total)
    block = min(256, own)

    def body(at, carry):
        slot = lax.rem(at, slots)
        for copy in copies(at, slot):
            copy.wait()

        @pl.when(at + slots - 1 < slabs)
        def _():
            for copy in copies(at + slots - 1, lax.rem(at + slots - 1, slots)):
                copy.start()

        here = pl.ds(pl.multiple_of(at * slab, slab), slab)
        for row in range(0, own, block):
            rows = slice(row, row + block)
            fill(table_ref, slab, c_buf.at[slot], d_buf.at[slot], hi_ref, lo_ref, at * slab, rows)
            total[:, rows] += multiply(left_c, left_s, hi_ref, lo_ref, here, rows)
        return carry

    lax.fori_loop(0, slabs, body, 0)
    new = complete(step_count, total[...], turned)
    for peer in range(out_ref.shape[0]):
        out_ref[peer] = new


def next_kernel(chunk, q_ref, z_ref, hi_ref, lo_ref, out_ref, left_c, left_s):
    _, _, new = advance(chunk, q_ref[0] + 1, z_ref, hi_ref, lo_ref, left_c, left_s)
    for peer in range(out_ref.shape[0]):
        out_ref[peer] = new


def last_kernel(chunk, q_ref, z_ref, hi_ref, lo_ref, out_ref, sums_ref, left_c, left_s):
    mine, turned, new = advance(chunk, q_ref[0] + 1, z_ref, hi_ref, lo_ref, left_c, left_s)
    out_ref[...] = new

    def summed(value):
        return jnp.sum(jnp.sum(value, axis=1, keepdims=True), axis=0, keepdims=True)

    row = lax.broadcasted_iota(jnp.int32, (SUB, LANE), 0)
    sums = jnp.where(row == 0, summed(new * new), 0.0)
    sums = sums + jnp.where(row == 1, summed(mine * new), 0.0)
    sums = sums + jnp.where(row == 2, summed(turned * new), 0.0)
    for peer in range(sums_ref.shape[0]):
        sums_ref[peer] = sums


def first(step, z, coupling, delays):
    own, nodes = coupling.shape
    slab, slots = min(SLAB, nodes), 2
    return pl.pallas_call(
        functools.partial(first_kernel, slab),
        out_shape=(
            pltpu.VMEM((2, own // LANE, nodes, LANE), HIGH),
            pltpu.VMEM((2, nodes, own), LOW),
            pltpu.VMEM(z.shape, F32),
        ),
        in_specs=[SMEM, VMEM, ANY, ANY],
        out_specs=(VMEM, VMEM, VMEM),
        scratch_shapes=[
            pltpu.VMEM((16, nodes), HIGH),
            pltpu.VMEM((16, nodes), HIGH),
            pltpu.VMEM((16, own), F32),
            pltpu.VMEM((4, SUB, LANE), F32),
            pltpu.VMEM((slots, own, slab), coupling.dtype),
            pltpu.VMEM((slots, own, slab), delays.dtype),
            pltpu.SemaphoreType.DMA((slots,)),
            pltpu.SemaphoreType.DMA((slots,)),
        ],
        compiler_params=pltpu.CompilerParams(vmem_limit_bytes=GRANT - 4 * math.prod(z.shape)),
        name="first",
    )(step, z, coupling, delays)


def apply(kernel, outputs, step, z, hi, lo):
    nodes = z.shape[0] * z.shape[2]
    return pl.pallas_call(
        functools.partial(kernel, min(CHUNK, nodes)),
        out_shape=tuple(pltpu.VMEM(shape, F32) for shape in outputs),
        in_specs=[SMEM, VMEM, VMEM, VMEM],
        out_specs=(VMEM,) * len(outputs),
        scratch_shapes=[pltpu.VMEM((16, nodes), HIGH), pltpu.VMEM((16, nodes), HIGH)],
        compiler_params=pltpu.CompilerParams(vmem_limit_bytes=GRANT),
        name="apply",
    )(step, z, hi, lo)


def finish_kernel(nodes, y_ref, sums_ref, vector_ref, value_ref):
    sums = jnp.sum(sums_ref[...], axis=0)
    vector_ref[...] = y_ref[...] * (1.0 / jnp.sqrt(sums[0:1, 0:1] / nodes + EPS))
    lane = lax.broadcasted_iota(jnp.int32, (1, LANE), 1)
    value_ref[...] = jnp.where(lane == 0, sums[1:2], sums[2:3]) * (1.0 / nodes)


def finish(nodes, y, sums):
    return pl.pallas_call(
        functools.partial(finish_kernel, nodes),
        out_shape=(jax.ShapeDtypeStruct(y.shape, F32), jax.ShapeDtypeStruct((1, LANE), F32)),
        in_specs=[VMEM, VMEM],
        out_specs=(VMEM, VMEM),
        name="finish",
    )(y, sums)


def copies_of_all(value):
    return lax.all_to_all(value, "rows", 0, 0, tiled=True)


def exchange(value):
    return in_vmem(copies_of_all(value))


def in_vmem(value):
    return pltpu.with_memory_space_constraint(value, pltpu.VMEM)


def solution(mesh):
    peers = mesh.shape["rows"]

    def point(coupling, delays, step, start):
        nodes = coupling.shape[1]
        z = exchange(jnp.broadcast_to(start[None], (peers, *start.shape)))
        hi, lo, y = first(step, z, coupling, delays)
        hi, lo = in_vmem(hi), in_vmem(lo)
        for sweep in range(1, ITERS - 1):
            (y,) = apply(next_kernel, [z.shape], step, exchange(y), hi, lo)
        y, sums = apply(last_kernel, [z.shape[1:], (peers, SUB, LANE)], step, exchange(y), hi, lo)
        return finish(nodes, y, exchange(sums))

    def shards(coupling, delays, freq_index, initial):
        vectors, values = [], []
        for at in range(freq_index.shape[0]):
            vector, value = point(coupling, delays, freq_index[at : at + 1], initial[at])
            vectors.append(vector)
            values.append(value[0, 0:2])
        return jnp.stack(vectors), jnp.stack(values)

    return jax.shard_map(
        shards,
        mesh=mesh,
        in_specs=(P("rows", None), P("rows", None), P("freq"), P("freq", None, "rows")),
        out_specs=(P("freq", None, "rows"), P("freq", None)),
        check_vma=False,
    )
```
